32 devices in a mesh: row: 4 (over z), col: 8 (over y, x, core).
Axes of the slice: x: 2, y: 2, z: 4, core: 2. Of those that a mesh axis runs over, the one named last changes fastest.
Arguments:
- green: float32 [512, 16384], P(('row', 'col')), may hold values from -0.375 to 0.375
- noise_precision: float32 [512], P(('row', 'col')), may hold values from 0.5 to 4
- data_set: int32 [512], P(('row', 'col')), may hold values from 0 to 3
- set_scale: float32 [4], replicated, may hold values from 0.5 to 2
- stiffness: float32 [8192], replicated, may hold values from 0.25 to 2
- patch_cell: int32 [8192], replicated, may hold values from 0 to 8191, each once
Outputs:
- precision_matrix: float32 [16384, 16384], P('row', 'col')
The draws below stay inside these ranges and needn't reach their ends.
Inputs may be any that keep to these rules, and one draw needn't show every extreme that they name: `patch_cell`: every cell 0 to 8191 holds exactly one patch.
All inputs are finite; a program needn't handle non-finite values.
Results may differ from the reference program's by a relative error of at most 0.00005.
Values sent between devices are 32-bit elements; how exact they have to be, the bound alone decides.
A program may use at most 256 MiB of HBM per device.

```python
import math
import jax
import jax.numpy as jnp
from jax import lax

NSTRIKE = 128
NDIP = 64
NSETS = 4
O = 512
P_SIZE = 8192
M = 16384


def place_ends(entries, stream_key, least, high):
    shape = entries.shape
    place = [jax.random.randint(jax.random.fold_in(stream_key, axis), (), 0, shape[axis]) for axis in range(len(shape))]
    entries = entries.at[tuple(place)].set(least)
    longest = shape.index(max(shape))
    place[longest] = (place[longest] + 1) % shape[longest]
    return entries.at[tuple(place)].set(high)


def levels(rng, shape, cuts, low, largest):
    def one(position, blocks):
        draws = jax.random.uniform(jax.random.fold_in(jax.random.fold_in(rng, 6), position), (blocks,), jnp.float32, low / len(cuts), largest / len(cuts))
        return jnp.repeat(jnp.exp(draws), shape[position] // blocks).reshape((-1,) + (1,) * (len(shape) - position - 1))

    level = one(*cuts[0])
    for cut in cuts[1:]:
        level = level * one(*cut)
    return level


def gaussian(key, extent, scale, bound, cuts=(), kind=jnp.bfloat16):
    result = scale * jax.random.normal(key, extent, jnp.float32)
    if cuts:
        result = result * levels(key, extent, cuts, -0.22, 0.18)
    return jnp.clip(result, -bound, bound).astype(kind)


def setup_inputs(seed: int = 0) -> dict:
    splits = jax.random.split(jax.random.key(seed), 7)
    return {
        "green": gaussian(splits[0], (O, M), (O // 2) ** -0.5, 0.375, ((0, 32),), jnp.float32),
        "noise_precision": jnp.clip(jnp.exp(math.log(4.0) - 2.0794415 * jax.random.uniform(splits[1], (O,), jnp.float32) ** levels(splits[1], (O,), ((0, 32),), -0.2, 0.2)), 0.5, 4.0),
        "data_set": place_ends(jax.random.randint(splits[2], (O,), 0, NSETS), jax.random.fold_in(splits[2], 1), 0, NSETS - 1).astype(jnp.int32),
        "set_scale": jnp.clip(jnp.exp(jax.random.uniform(splits[3], (NSETS,), jnp.float32, math.log(0.5), math.log(2.0))), 0.5, 2.0),
        "stiffness": jnp.clip(jnp.exp(jax.random.uniform(splits[4], (P_SIZE,), jnp.float32, math.log(0.25), math.log(2.0))), 0.25, 2.0),
        "patch_cell": jax.random.permutation(splits[5], P_SIZE).astype(jnp.int32),
    }


def reference(green, noise_precision, data_set, set_scale, stiffness, patch_cell):
    weight = noise_precision * set_scale[data_set]
    scaled = green * jnp.sqrt(weight)[:, None]
    precision_matrix = lax.dot_general(scaled, scaled, (((0,), (0,)), ((), ())), precision=lax.Precision.HIGHEST, preferred_element_type=jnp.float32)
    patch_count = NSTRIKE * NDIP
    cell_ids = jnp.arange(patch_count, dtype=jnp.int32)
    owner = jnp.zeros((patch_count,), jnp.int32).at[patch_cell].set(cell_ids)
    strike_pos = cell_ids // NDIP
    dip_pos = cell_ids % NDIP
    along = owner[jnp.minimum(cell_ids + NDIP, patch_count - 1)]
    below = owner[jnp.minimum(cell_ids + 1, patch_count - 1)]
    heads = jnp.concatenate([owner, owner])
    tails = jnp.concatenate([along, below])
    valid = jnp.concatenate([strike_pos < NSTRIKE - 1, dip_pos < NDIP - 1])
    edges = jnp.where(valid, 0.5 * (stiffness[heads] + stiffness[tails]), 0.0)
    row_list = []
    col_list = []
    values = []
    for component in range(2):
        first_ids = (component * patch_count + heads).astype(jnp.int32)
        second_ids = (component * patch_count + tails).astype(jnp.int32)
        row_list += [first_ids, second_ids, first_ids, second_ids]
        col_list += [second_ids, first_ids, first_ids, second_ids]
        values += [-edges, -edges, edges, edges]
    return precision_matrix.at[jnp.concatenate(row_list), jnp.concatenate(col_list)].add(jnp.concatenate(values))
```

```python
import jax
import jax.numpy as jnp
from jax import lax
from jax.experimental import pallas as pl
from jax.experimental.pallas import tpu as pltpu
from jax.sharding import PartitionSpec as P

NSTRIKE = 128
NDIP = 64
LANES = 128
VMEM_GRANT = 16 * 2**20
MESH = pl.DeviceIdType.MESH


def xor(value, other, count):
    total = 0
    bit = 1
    while bit < count:
        total = total + ((value // bit) % 2 + (other // bit) % 2) % 2 * bit
        bit *= 2
    return total


def ring_chip(place, chips):
    return jnp.where(place < chips // 2, place, chips + chips // 2 - 1 - place)


def plane_at(row, order, row_count):
    low = jnp.where(order % 2 == 1, row - (order + 1) // 2, row + order // 2)
    near = jnp.minimum(row, row_count - 1 - row)
    far = jnp.where(row < row_count - 1 - row, order, row_count - 1 - order)
    return jnp.where(order <= 2 * near, low, far)


def split_two(values):
    high = values.astype(jnp.bfloat16)
    low = (values - high.astype(jnp.float32)).astype(jnp.bfloat16)
    return high, low


def split_three(values):
    high = values.astype(jnp.bfloat16)
    rest = values - high.astype(jnp.float32)
    middle = rest.astype(jnp.bfloat16)
    low = (rest - middle.astype(jnp.float32)).astype(jnp.bfloat16)
    return high, middle, low


def contract_rows(left, right):
    return lax.dot_general(left, right, (((0,), (0,)), ((), ())), preferred_element_type=jnp.float32)


def load_right(col, plane, right):
    depth = col.shape[1]
    high, low = split_two(col[plane])
    right[pl.ds(0, depth), :] = high
    right[pl.ds(depth, depth), :] = high
    right[pl.ds(2 * depth, depth), :] = low


def strip_left(rowp, plane, start, height):
    width = rowp.shape[3]
    half = start // width
    first = pl.multiple_of(start % width, LANES)
    high, low = split_two(rowp[half, plane, :, pl.ds(first, height)])
    return jnp.concatenate([high, low, high], axis=0)


def code_of(cells):
    return ((cells // NDIP) * (2 * NDIP) + cells % NDIP).astype(jnp.float32)


def hot_strike(cells):
    ids = lax.broadcasted_iota(jnp.int32, (NSTRIKE, LANES), 0)
    return jnp.where(ids == cells // NDIP, 1.0, 0.0)


def hot_dip(cells):
    ids = lax.broadcasted_iota(jnp.int32, (LANES, LANES), 0)
    return ids == cells % NDIP


def degree_grid(stiff, cell):
    lines = cell.shape[0]

    def add(step, total):
        strike = hot_strike(cell[pl.ds(step, 1), :]).astype(jnp.bfloat16)
        hot = hot_dip(cell[pl.ds(step, 1), :])
        parts = split_three(jnp.where(hot, stiff[pl.ds(step, 1), :], 0.0))
        return total + lax.dot_general(
            strike,
            jnp.concatenate(parts, axis=0),
            (((1,), (1,)), ((), ())),
            preferred_element_type=jnp.float32,
        )

    sums = lax.fori_loop(0, lines, add, jnp.zeros((NSTRIKE, 3 * LANES), jnp.float32))
    grid = sums[:, :LANES] + sums[:, LANES : 2 * LANES] + sums[:, 2 * LANES :]
    strike_ids = lax.broadcasted_iota(jnp.int32, (NSTRIKE, LANES), 0)
    dip_ids = lax.broadcasted_iota(jnp.int32, (NSTRIKE, LANES), 1)
    degree = jnp.where(strike_ids < NSTRIKE - 1, 0.5 * (grid + pltpu.roll(grid, NSTRIKE - 1, 0)), 0.0)
    degree = degree + jnp.where(strike_ids > 0, 0.5 * (grid + pltpu.roll(grid, 1, 0)), 0.0)
    degree = degree + jnp.where(dip_ids < NDIP - 1, 0.5 * (grid + pltpu.roll(grid, LANES - 1, 1)), 0.0)
    degree = degree + jnp.where(dip_ids > 0, 0.5 * (grid + pltpu.roll(grid, 1, 1)), 0.0)
    return degree


def degree_line(parts, cells):
    strike = hot_strike(cells).astype(jnp.bfloat16)
    table = contract_rows(parts[0], strike) + contract_rows(parts[1], strike) + contract_rows(parts[2], strike)
    return jnp.sum(jnp.where(hot_dip(cells), table, 0.0), axis=0, keepdims=True)


def prior_strip(stiff, cell, acc, row_line, col_line, start, height, same):
    width = acc.shape[1]

    @pl.when(same)
    def _():
        @pl.loop(0, height // LANES)
        def _(block):
            first = pl.multiple_of(start + block * LANES, LANES)
            line = row_line + first // LANES
            full = (LANES, LANES)
            row_code = jnp.broadcast_to(code_of(cell[pl.ds(line, 1), :]), full).T
            row_half = jnp.broadcast_to(-0.5 * stiff[pl.ds(line, 1), :], full).T
            for place in range(width // LANES):
                other = col_line + place
                apart = jnp.abs(row_code - code_of(cell[pl.ds(other, 1), :]))
                edge = row_half - 0.5 * stiff[pl.ds(other, 1), :]
                near = (apart == 1.0) | (apart == 2.0 * NDIP)
                acc[pl.ds(first, LANES), pl.ds(place * LANES, LANES)] = jnp.where(near, edge, 0.0)

    @pl.when(jnp.logical_not(same))
    def _():
        acc[pl.ds(start, height), :] = jnp.zeros((height, width), jnp.float32)


def gather_kernel(
    row_count,
    col_count,
    green,
    noise,
    data_set,
    set_scale,
    stiff,
    cell,
    acc,
    rowp,
    col,
    scaled,
    right,
    send_plane,
    recv_plane,
    send_up,
    send_down,
    recv_z,
    send_cw,
    send_ccw,
    recv_ring,
    send_core,
    recv_core,
):
    row = lax.axis_index("row")
    me = lax.axis_index("col")
    core = me % 2
    chip = me // 2
    chips = col_count // 2
    rows, order_full = green.shape
    height, width = acc.shape
    patches = stiff.shape[0] * LANES
    owner = chip == row
    home = 2 * row + core
    partner = 2 * chip + 1 - core
    place = ring_chip(chip, chips)
    hop_cw = lax.rem(place - ring_chip(row, chips) + chips, chips)
    hop_ccw = lax.rem(chips - hop_cw, chips)
    next_cw = 2 * ring_chip(lax.rem(place + 1, chips), chips) + core
    next_ccw = 2 * ring_chip(lax.rem(place + chips - 1, chips), chips) + core
    has_up = row + 1 < row_count
    has_down = row > 0
    above = jnp.minimum(row + 1, row_count - 1)
    below = jnp.maximum(row - 1, 0)

    barrier = pltpu.get_barrier_semaphore()
    for step in range(1, col_count):
        pl.semaphore_signal(barrier, inc=1, device_id=(row, xor(me, step, col_count)), device_id_type=MESH)

    @pl.when(has_up)
    def _():
        pl.semaphore_signal(barrier, inc=1, device_id=(above, me), device_id_type=MESH)

    @pl.when(has_down)
    def _():
        pl.semaphore_signal(barrier, inc=1, device_id=(below, me), device_id_type=MESH)

    row_ids = lax.broadcasted_iota(jnp.int32, (rows, LANES), 0)
    weight = jnp.zeros((rows, LANES), jnp.float32)
    for entry in range(rows):
        weight = jnp.where(row_ids == entry, noise[entry] * set_scale[data_set[entry]], weight)
    factor = jnp.sqrt(weight)

    @pl.loop(0, order_full // LANES)
    def _(step):
        lanes = pl.ds(pl.multiple_of(step * LANES, LANES), LANES)
        scaled[:, lanes] = green[:, lanes] * factor

    def slab(index):
        return pl.ds(pl.multiple_of(index * rows, rows), rows)

    own = pl.ds(pl.multiple_of(me * width, LANES), width)
    col[row, slab(me), :] = scaled[:, own]
    pl.semaphore_wait(barrier, col_count - 1 + has_up.astype(jnp.int32) + has_down.astype(jnp.int32))

    def plane_copy(step):
        target = xor(me, step, col_count)
        return pltpu.make_async_remote_copy(
            src_ref=scaled.at[:, pl.ds(pl.multiple_of(target * width, LANES), width)],
            dst_ref=col.at[row, slab(me), :],
            send_sem=send_plane.at[step],
            recv_sem=recv_plane.at[step],
            device_id=(row, target),
            device_id_type=MESH,
        )

    for step in range(1, col_count):
        plane_copy(step).start()

    def z_copy(plane, step, up):
        where = slab(xor(me, step, col_count))
        return pltpu.make_async_remote_copy(
            src_ref=col.at[plane, where, :],
            dst_ref=col.at[plane, where, :],
            send_sem=send_up.at[plane] if up else send_down.at[plane],
            recv_sem=recv_z.at[plane, step],
            device_id=(above if up else below, me),
            device_id_type=MESH,
        )

    def ring_copy(plane, step, clockwise, source):
        where = slab(xor(home, step, col_count))
        return pltpu.make_async_remote_copy(
            src_ref=source.at[plane, where, :],
            dst_ref=rowp.at[core, plane, where, :],
            send_sem=send_cw.at[plane] if clockwise else send_ccw.at[plane],
            recv_sem=recv_ring.at[plane, step],
            device_id=(row, next_cw if clockwise else next_ccw),
            device_id_type=MESH,
        )

    def core_copy(plane, step, source):
        where = slab(xor(home, step, col_count))
        return pltpu.make_async_remote_copy(
            src_ref=source.at[plane, where, :],
            dst_ref=rowp.at[core, plane, where, :],
            send_sem=send_core.at[plane],
            recv_sem=recv_core.at[plane],
            device_id=(row, partner),
            device_id_type=MESH,
        )

    def arrived(plane, step):
        @pl.when(has_up & (plane <= row))
        def _():
            z_copy(plane, step, True).start()

        @pl.when(has_down & (plane >= row))
        def _():
            z_copy(plane, step, False).start()

        @pl.when(owner)
        def _():
            @pl.when(step % 2 == 0)
            def _():
                ring_copy(plane, step, True, col).start()

            @pl.when(step % 2 == 1)
            def _():
                ring_copy(plane, step, False, col).start()

            core_copy(plane, step, col).start()
            where = slab(xor(home, step, col_count))
            rowp[core, plane, where, :] = col[plane, where, :]

    held = rowp.at[core]

    def ring_step(plane, step, hop, clockwise):
        ring_copy(plane, step, clockwise, held).wait_recv()

        @pl.when(hop < chips - 1)
        def _():
            ring_copy(plane, step, clockwise, held).start()

        core_copy(plane, step, held).start()

    def both_sides(distance, act):
        @pl.when(row - distance >= 0)
        def _():
            act(row - distance)

        @pl.when((distance > 0) & (row + distance < row_count))
        def _():
            act(row + distance)

    def wait_core(plane):
        whole = rowp.at[1 - core, plane]
        pltpu.make_async_remote_copy(
            src_ref=whole,
            dst_ref=whole,
            send_sem=send_core.at[plane],
            recv_sem=recv_core.at[plane],
            device_id=(row, partner),
            device_id_type=MESH,
        ).wait_recv()

    lag = 2 * (chips - 1)
    steps = row_count * col_count
    strip = height // col_count
    same = (row * height) // patches == (me * width) // patches
    row_line = lax.rem(row * height, patches) // LANES
    col_line = lax.rem(me * width, patches) // LANES

    @pl.loop(0, steps + lag)
    def _(now):
        distance = now // col_count
        step = lax.rem(now, col_count)

        @pl.when((now > 0) & (now < col_count))
        def _():
            pltpu.make_async_remote_copy(
                src_ref=col.at[row, slab(xor(me, step, col_count)), :],
                dst_ref=col.at[row, slab(xor(me, step, col_count)), :],
                send_sem=send_plane.at[step],
                recv_sem=recv_plane.at[step],
                device_id=(row, partner),
                device_id_type=MESH,
            ).wait_recv()

        @pl.when(now < steps)
        def _():
            def receive(plane):
                @pl.when(now >= col_count)
                def _():
                    z_copy(plane, step, True).wait_recv()

                arrived(plane, step)

            both_sides(distance, receive)

        def ring_turn(hop, clockwise):
            late = now - 2 * hop

            @pl.when((hop > 0) & (late >= 0) & (late < steps))
            def _():
                both_sides(
                    late // col_count,
                    lambda plane: ring_step(plane, lax.rem(late, col_count), hop, clockwise),
                )

        @pl.when(now % 2 == 0)
        def _():
            ring_turn(hop_cw, True)

        @pl.when(now % 2 == 1)
        def _():
            ring_turn(hop_ccw, False)

        @pl.when(now < col_count)
        def _():
            prior_strip(stiff, cell, acc, row_line, col_line, pl.multiple_of(step * strip, LANES), strip, same)

        @pl.when((now == col_count) & owner)
        def _():
            parts = split_three(degree_grid(stiff, cell))
            corner = lax.broadcasted_iota(jnp.int32, (LANES, LANES), 0) == lax.broadcasted_iota(
                jnp.int32, (LANES, LANES), 1
            )

            @pl.loop(0, width // LANES)
            def _(block):
                line = degree_line(parts, cell[pl.ds(col_line + block, 1), :])
                across = pl.ds(pl.multiple_of(block * LANES, LANES), LANES)
                down = pl.ds(pl.multiple_of(core * width + block * LANES, LANES), LANES)
                acc[down, across] = acc[down, across] + jnp.where(corner, line, 0.0)

        turn = now - col_count - lag

        @pl.when(turn >= 0)
        def _():
            plane = plane_at(row, turn // col_count, row_count)
            part = lax.rem(turn, col_count)

            @pl.when(part == 0)
            def _():
                wait_core(plane)
                load_right(col, plane, right)

            start = pl.multiple_of(part * strip, LANES)
            left = strip_left(rowp, plane, start, strip)
            piece = min(width, 512)

            @pl.loop(0, width // piece)
            def _(block):
                across = pl.ds(pl.multiple_of(block * piece, LANES), piece)
                down = pl.ds(start, strip)
                acc[down, across] = acc[down, across] + contract_rows(left, right[:, across])

    wait_core(plane_at(row, row_count - 1, row_count))

    for step in range(1, col_count):
        plane_copy(step).wait_send()

    @pl.loop(0, row_count)
    def _(plane):
        whole = col.at[plane]
        half = whole.at[pl.ds(0, whole.shape[0] // 2), :]

        def sent(ref, sem):
            pltpu.make_async_remote_copy(
                src_ref=ref,
                dst_ref=ref,
                send_sem=sem,
                recv_sem=recv_core.at[plane],
                device_id=(row, partner),
                device_id_type=MESH,
            ).wait_send()

        sent(whole, send_core.at[plane])

        @pl.when(has_up & (plane <= row))
        def _():
            sent(whole, send_up.at[plane])

        @pl.when(has_down & (plane >= row))
        def _():
            sent(whole, send_down.at[plane])

        @pl.when(hop_cw < chips - 1)
        def _():
            sent(half, send_cw.at[plane])

        @pl.when(hop_ccw < chips - 1)
        def _():
            sent(half, send_ccw.at[plane])


def gather_and_sum(row_count, col_count, green, noise, data_set, set_scale, stiff, cell):
    rows, order_full = green.shape
    height = order_full // row_count
    width = order_full // col_count
    depth = col_count * rows
    vmem = pl.BlockSpec(memory_space=pltpu.VMEM)
    smem = pl.BlockSpec(memory_space=pltpu.SMEM)
    dma = pltpu.SemaphoreType.DMA

    def body(*refs):
        gather_kernel(row_count, col_count, *refs)

    return pl.pallas_call(
        body,
        out_shape=(
            pltpu.VMEM((height, width), jnp.float32),
            pltpu.VMEM((2, row_count, depth, width), jnp.float32),
            pltpu.VMEM((row_count, depth, width), jnp.float32),
        ),
        in_specs=[vmem, smem, smem, smem, vmem, vmem],
        out_specs=(vmem, vmem, vmem),
        scratch_shapes=[
            pltpu.VMEM((rows, order_full), jnp.float32),
            pltpu.VMEM((3 * depth, width), jnp.bfloat16),
            dma((col_count,)),
            dma((col_count,)),
            dma((row_count,)),
            dma((row_count,)),
            dma((row_count, col_count)),
            dma((row_count,)),
            dma((row_count,)),
            dma((row_count, col_count)),
            dma((row_count,)),
            dma((row_count,)),
        ],
        compiler_params=pltpu.CompilerParams(
            collective_id=0, has_side_effects=True, vmem_limit_bytes=VMEM_GRANT
        ),
    )(green, noise, data_set, set_scale, stiff, cell)


def finish_kernel(row_count, slots, acc, rowp, col, out, stage, right, sems):
    row = lax.axis_index("row")
    plane = plane_at(row, row_count - 1, row_count)
    height, width = acc.shape
    strip = stage.shape[1]
    piece = min(width, 512)
    load_right(col, plane, right)

    def copy(index, slot):
        start = pl.multiple_of(index * strip, LANES)
        return pltpu.make_async_copy(stage.at[slot], out.at[pl.ds(start, strip), :], sems.at[slot])

    count = height // strip

    @pl.loop(0, count)
    def _(index):
        slot = lax.rem(index, slots)

        @pl.when(index >= slots)
        def _():
            copy(index - slots, slot).wait()

        start = pl.multiple_of(index * strip, LANES)
        left = strip_left(rowp, plane, start, strip)

        @pl.loop(0, width // piece)
        def _(block):
            across = pl.ds(pl.multiple_of(block * piece, LANES), piece)
            stage[slot, :, across] = acc[pl.ds(start, strip), across] + contract_rows(left, right[:, across])

        copy(index, slot).start()

    for back in range(slots):
        index = count - slots + back
        copy(index, index % slots).wait()


def finish(row_count, acc, rowp, col):
    height, width = acc.shape
    depth = col.shape[1]
    vmem = pl.BlockSpec(memory_space=pltpu.VMEM)
    strip = min(height, 256)
    slots = 4

    def body(*refs):
        finish_kernel(row_count, slots, *refs)

    return pl.pallas_call(
        body,
        out_shape=jax.ShapeDtypeStruct((height, width), jnp.float32),
        in_specs=[vmem, vmem, vmem],
        out_specs=pl.BlockSpec(memory_space=pl.ANY),
        scratch_shapes=[
            pltpu.VMEM((slots, strip, width), jnp.float32),
            pltpu.VMEM((3 * depth, width), jnp.bfloat16),
            pltpu.SemaphoreType.DMA((slots,)),
        ],
        compiler_params=pltpu.CompilerParams(vmem_limit_bytes=VMEM_GRANT),
    )(*(pltpu.with_memory_space_constraint(array, pltpu.VMEM) for array in (acc, rowp, col)))


def per_device(green, noise_precision, data_set, set_scale, stiffness, patch_cell):
    row_count = lax.axis_size("row")
    col_count = lax.axis_size("col")
    lines = stiffness.shape[0] // LANES
    acc, rowp, col = gather_and_sum(
        row_count,
        col_count,
        green,
        noise_precision,
        data_set,
        set_scale,
        stiffness.reshape(lines, LANES),
        patch_cell.reshape(lines, LANES),
    )
    return finish(row_count, acc, rowp, col)


def solution(mesh):
    placed = (P(("row", "col"), None), P(("row", "col")), P(("row", "col")), P(), P(), P())
    return jax.shard_map(
        per_device, mesh=mesh, in_specs=placed, out_specs=P("row", "col"), check_vma=False
    )
```

```python
import jax
import jax.numpy as jnp
from jax import lax
from jax.experimental import pallas as pl
from jax.experimental.pallas import tpu as pltpu
from jax.sharding import PartitionSpec as P

NSTRIKE = 128
NDIP = 64
LANES = 128
VMEM_GRANT = 16 * 2**20
MESH = pl.DeviceIdType.MESH


def xor(value, other, count):
    total = 0
    bit = 1
    while bit < count:
        total = total + ((value // bit) % 2 + (other // bit) % 2) % 2 * bit
        bit *= 2
    return total


def ring_chip(place, chips):
    return jnp.where(place < chips // 2, place, chips + chips // 2 - 1 - place)


def plane_at(row, order, row_count):
    low = jnp.where(order % 2 == 1, row - (order + 1) // 2, row + order // 2)
    near = jnp.minimum(row, row_count - 1 - row)
    far = jnp.where(row < row_count - 1 - row, order, row_count - 1 - order)
    return jnp.where(order <= 2 * near, low, far)


def split_two(values):
    high = values.astype(jnp.bfloat16)
    low = (values - high.astype(jnp.float32)).astype(jnp.bfloat16)
    return high, low


def split_three(values):
    high = values.astype(jnp.bfloat16)
    rest = values - high.astype(jnp.float32)
    middle = rest.astype(jnp.bfloat16)
    low = (rest - middle.astype(jnp.float32)).astype(jnp.bfloat16)
    return high, middle, low


def contract_rows(left, right):
    return lax.dot_general(left, right, (((0,), (0,)), ((), ())), preferred_element_type=jnp.float32)


def load_right(col, plane, right):
    depth = col.shape[1]
    high, low = split_two(col[plane])
    right[pl.ds(0, depth), :] = high
    right[pl.ds(depth, depth), :] = high
    right[pl.ds(2 * depth, depth), :] = low


def strip_left(rowp, plane, start, height):
    width = rowp.shape[3]
    half = start // width
    first = pl.multiple_of(start % width, LANES)
    high, low = split_two(rowp[half, plane, :, pl.ds(first, height)])
    return jnp.concatenate([high, low, high], axis=0)


def code_of(cells):
    return ((cells // NDIP) * (2 * NDIP) + cells % NDIP).astype(jnp.float32)


def hot_strike(cells):
    ids = lax.broadcasted_iota(jnp.int32, (NSTRIKE, LANES), 0)
    return jnp.where(ids == cells // NDIP, 1.0, 0.0)


def hot_dip(cells):
    ids = lax.broadcasted_iota(jnp.int32, (LANES, LANES), 0)
    return ids == cells % NDIP


def degree_grid(stiff, cell):
    lines = cell.shape[0]

    def add(step, total):
        strike = hot_strike(cell[pl.ds(step, 1), :]).astype(jnp.bfloat16)
        hot = hot_dip(cell[pl.ds(step, 1), :])
        parts = split_three(jnp.where(hot, stiff[pl.ds(step, 1), :], 0.0))
        return total + lax.dot_general(
            strike,
            jnp.concatenate(parts, axis=0),
            (((1,), (1,)), ((), ())),
            preferred_element_type=jnp.float32,
        )

    sums = lax.fori_loop(0, lines, add, jnp.zeros((NSTRIKE, 3 * LANES), jnp.float32))
    grid = sums[:, :LANES] + sums[:, LANES : 2 * LANES] + sums[:, 2 * LANES :]
    strike_ids = lax.broadcasted_iota(jnp.int32, (NSTRIKE, LANES), 0)
    dip_ids = lax.broadcasted_iota(jnp.int32, (NSTRIKE, LANES), 1)
    degree = jnp.where(strike_ids < NSTRIKE - 1, 0.5 * (grid + pltpu.roll(grid, NSTRIKE - 1, 0)), 0.0)
    degree = degree + jnp.where(strike_ids > 0, 0.5 * (grid + pltpu.roll(grid, 1, 0)), 0.0)
    degree = degree + jnp.where(dip_ids < NDIP - 1, 0.5 * (grid + pltpu.roll(grid, LANES - 1, 1)), 0.0)
    degree = degree + jnp.where(dip_ids > 0, 0.5 * (grid + pltpu.roll(grid, 1, 1)), 0.0)
    return degree


def degree_line(parts, cells):
    strike = hot_strike(cells).astype(jnp.bfloat16)
    table = contract_rows(parts[0], strike) + contract_rows(parts[1], strike) + contract_rows(parts[2], strike)
    return jnp.sum(jnp.where(hot_dip(cells), table, 0.0), axis=0, keepdims=True)


def prior_strip(stiff, cell, acc, row_line, col_line, start, height, same):
    width = acc.shape[1]

    @pl.when(same)
    def _():
        @pl.loop(0, height // LANES)
        def _(block):
            first = pl.multiple_of(start + block * LANES, LANES)
            line = row_line + first // LANES
            full = (LANES, LANES)
            row_code = jnp.broadcast_to(code_of(cell[pl.ds(line, 1), :]), full).T
            row_half = jnp.broadcast_to(-0.5 * stiff[pl.ds(line, 1), :], full).T
            for place in range(width // LANES):
                other = col_line + place
                apart = jnp.abs(row_code - code_of(cell[pl.ds(other, 1), :]))
                edge = row_half - 0.5 * stiff[pl.ds(other, 1), :]
                near = (apart == 1.0) | (apart == 2.0 * NDIP)
                acc[pl.ds(first, LANES), pl.ds(place * LANES, LANES)] = jnp.where(near, edge, 0.0)

    @pl.when(jnp.logical_not(same))
    def _():
        acc[pl.ds(start, height), :] = jnp.zeros((height, width), jnp.float32)


def gather_kernel(
    row_count,
    col_count,
    green,
    noise,
    data_set,
    set_scale,
    stiff,
    cell,
    acc,
    rowp,
    col,
    scaled,
    right,
    send_plane,
    recv_plane,
    send_up,
    send_down,
    recv_z,
    send_cw,
    send_ccw,
    recv_ring,
    send_core,
    recv_core,
):
    row = lax.axis_index("row")
    me = lax.axis_index("col")
    core = me % 2
    chip = me // 2
    chips = col_count // 2
    rows, order_full = green.shape
    height, width = acc.shape
    patches = stiff.shape[0] * LANES
    owner = chip == row
    home = 2 * row + core
    partner = 2 * chip + 1 - core
    place = ring_chip(chip, chips)
    hop_cw = lax.rem(place - ring_chip(row, chips) + chips, chips)
    hop_ccw = lax.rem(chips - hop_cw, chips)
    next_cw = 2 * ring_chip(lax.rem(place + 1, chips), chips) + core
    next_ccw = 2 * ring_chip(lax.rem(place + chips - 1, chips), chips) + core
    has_up = row + 1 < row_count
    has_down = row > 0
    above = jnp.minimum(row + 1, row_count - 1)
    below = jnp.maximum(row - 1, 0)

    barrier = pltpu.get_barrier_semaphore()
    for step in range(1, col_count):
        pl.semaphore_signal(barrier, inc=1, device_id=(row, xor(me, step, col_count)), device_id_type=MESH)

    @pl.when(has_up)
    def _():
        pl.semaphore_signal(barrier, inc=1, device_id=(above, me), device_id_type=MESH)

    @pl.when(has_down)
    def _():
        pl.semaphore_signal(barrier, inc=1, device_id=(below, me), device_id_type=MESH)

    row_ids = lax.broadcasted_iota(jnp.int32, (rows, LANES), 0)
    weight = jnp.zeros((rows, LANES), jnp.float32)
    for entry in range(rows):
        weight = jnp.where(row_ids == entry, noise[entry] * set_scale[data_set[entry]], weight)
    factor = jnp.sqrt(weight)

    @pl.loop(0, order_full // LANES)
    def _(step):
        lanes = pl.ds(pl.multiple_of(step * LANES, LANES), LANES)
        scaled[:, lanes] = green[:, lanes] * factor

    def slab(index):
        return pl.ds(pl.multiple_of(index * rows, rows), rows)

    own = pl.ds(pl.multiple_of(me * width, LANES), width)
    col[row, slab(me), :] = scaled[:, own]
    pl.semaphore_wait(barrier, col_count - 1 + has_up.astype(jnp.int32) + has_down.astype(jnp.int32))

    def plane_copy(step):
        target = xor(me, step, col_count)
        return pltpu.make_async_remote_copy(
            src_ref=scaled.at[:, pl.ds(pl.multiple_of(target * width, LANES), width)],
            dst_ref=col.at[row, slab(me), :],
            send_sem=send_plane.at[step],
            recv_sem=recv_plane.at[step],
            device_id=(row, target),
            device_id_type=MESH,
        )

    for step in range(1, col_count):
        plane_copy(step).start()

    def z_copy(plane, step, up):
        where = slab(xor(me, step, col_count))
        return pltpu.make_async_remote_copy(
            src_ref=col.at[plane, where, :],
            dst_ref=col.at[plane, where, :],
            send_sem=send_up.at[plane] if up else send_down.at[plane],
            recv_sem=recv_z.at[plane, step],
            device_id=(above if up else below, me),
            device_id_type=MESH,
        )

    def ring_copy(plane, step, clockwise, source):
        where = slab(xor(home, step, col_count))
        return pltpu.make_async_remote_copy(
            src_ref=source.at[plane, where, :],
            dst_ref=rowp.at[core, plane, where, :],
            send_sem=send_cw.at[plane] if clockwise else send_ccw.at[plane],
            recv_sem=recv_ring.at[plane, step],
            device_id=(row, next_cw if clockwise else next_ccw),
            device_id_type=MESH,
        )

    def core_copy(plane, step, source):
        where = slab(xor(home, step, col_count))
        return pltpu.make_async_remote_copy(
            src_ref=source.at[plane, where, :],
            dst_ref=rowp.at[core, plane, where, :],
            send_sem=send_core.at[plane],
            recv_sem=recv_core.at[plane],
            device_id=(row, partner),
            device_id_type=MESH,
        )

    def arrived(plane, step):
        @pl.when(has_up & (plane <= row))
        def _():
            z_copy(plane, step, True).start()

        @pl.when(has_down & (plane >= row))
        def _():
            z_copy(plane, step, False).start()

        @pl.when(owner)
        def _():
            @pl.when(step % 2 == 0)
            def _():
                ring_copy(plane, step, True, col).start()

            @pl.when(step % 2 == 1)
            def _():
                ring_copy(plane, step, False, col).start()

            core_copy(plane, step, col).start()
            where = slab(xor(home, step, col_count))
            rowp[core, plane, where, :] = col[plane, where, :]

    held = rowp.at[core]

    def ring_step(plane, step, hop, clockwise):
        ring_copy(plane, step, clockwise, held).wait_recv()

        @pl.when(hop < chips - 1)
        def _():
            ring_copy(plane, step, clockwise, held).start()

        core_copy(plane, step, held).start()

    def both_sides(distance, act):
        @pl.when(row - distance >= 0)
        def _():
            act(row - distance)

        @pl.when((distance > 0) & (row + distance < row_count))
        def _():
            act(row + distance)

    def wait_core(plane):
        whole = rowp.at[1 - core, plane]
        pltpu.make_async_remote_copy(
            src_ref=whole,
            dst_ref=whole,
            send_sem=send_core.at[plane],
            recv_sem=recv_core.at[plane],
            device_id=(row, partner),
            device_id_type=MESH,
        ).wait_recv()

    lag = 2 * (chips - 1)
    steps = row_count * col_count
    strip = height // col_count
    same = (row * height) // patches == (me * width) // patches
    row_line = lax.rem(row * height, patches) // LANES
    col_line = lax.rem(me * width, patches) // LANES

    @pl.loop(0, steps + lag)
    def _(now):
        distance = now // col_count
        step = lax.rem(now, col_count)

        @pl.when((now > 0) & (now < col_count))
        def _():
            pltpu.make_async_remote_copy(
                src_ref=col.at[row, slab(xor(me, step, col_count)), :],
                dst_ref=col.at[row, slab(xor(me, step, col_count)), :],
                send_sem=send_plane.at[step],
                recv_sem=recv_plane.at[step],
                device_id=(row, partner),
                device_id_type=MESH,
            ).wait_recv()

        @pl.when(now < steps)
        def _():
            def receive(plane):
                @pl.when(now >= col_count)
                def _():
                    z_copy(plane, step, True).wait_recv()

                arrived(plane, step)

            both_sides(distance, receive)

        def ring_turn(hop, clockwise):
            late = now - 2 * hop

            @pl.when((hop > 0) & (late >= 0) & (late < steps))
            def _():
                both_sides(
                    late // col_count,
                    lambda plane: ring_step(plane, lax.rem(late, col_count), hop, clockwise),
                )

        @pl.when(now % 2 == 0)
        def _():
            ring_turn(hop_cw, True)

        @pl.when(now % 2 == 1)
        def _():
            ring_turn(hop_ccw, False)

        @pl.when(now < col_count)
        def _():
            prior_strip(stiff, cell, acc, row_line, col_line, pl.multiple_of(step * strip, LANES), strip, same)

        @pl.when((now == col_count) & owner)
        def _():
            parts = split_three(degree_grid(stiff, cell))
            corner = lax.broadcasted_iota(jnp.int32, (LANES, LANES), 0) == lax.broadcasted_iota(
                jnp.int32, (LANES, LANES), 1
            )

            @pl.loop(0, width // LANES)
            def _(block):
                line = degree_line(parts, cell[pl.ds(col_line + block, 1), :])
                across = pl.ds(pl.multiple_of(block * LANES, LANES), LANES)
                down = pl.ds(pl.multiple_of(core * width + block * LANES, LANES), LANES)
                acc[down, across] = acc[down, across] + jnp.where(corner, line, 0.0)

        turn = now - col_count - lag

        @pl.when(turn >= 0)
        def _():
            plane = plane_at(row, turn // col_count, row_count)
            part = lax.rem(turn, col_count)

            @pl.when(part == 0)
            def _():
                wait_core(plane)
                load_right(col, plane, right)

            piece = min(strip, 2 * LANES)

            @pl.loop(0, strip // piece)
            def _(block):
                start = pl.multiple_of(part * strip + block * piece, LANES)
                left = strip_left(rowp, plane, start, piece)
                acc[pl.ds(start, piece), :] = acc[pl.ds(start, piece), :] + contract_rows(left, right[...])

    wait_core(plane_at(row, row_count - 1, row_count))

    for step in range(1, col_count):
        plane_copy(step).wait_send()

    @pl.loop(0, row_count)
    def _(plane):
        whole = col.at[plane]
        half = whole.at[pl.ds(0, whole.shape[0] // 2), :]

        def sent(ref, sem):
            pltpu.make_async_remote_copy(
                src_ref=ref,
                dst_ref=ref,
                send_sem=sem,
                recv_sem=recv_core.at[plane],
                device_id=(row, partner),
                device_id_type=MESH,
            ).wait_send()

        sent(whole, send_core.at[plane])

        @pl.when(has_up & (plane <= row))
        def _():
            sent(whole, send_up.at[plane])

        @pl.when(has_down & (plane >= row))
        def _():
            sent(whole, send_down.at[plane])

        @pl.when(hop_cw < chips - 1)
        def _():
            sent(half, send_cw.at[plane])

        @pl.when(hop_ccw < chips - 1)
        def _():
            sent(half, send_ccw.at[plane])


def gather_and_sum(row_count, col_count, green, noise, data_set, set_scale, stiff, cell):
    rows, order_full = green.shape
    height = order_full // row_count
    width = order_full // col_count
    depth = col_count * rows
    vmem = pl.BlockSpec(memory_space=pltpu.VMEM)
    smem = pl.BlockSpec(memory_space=pltpu.SMEM)
    dma = pltpu.SemaphoreType.DMA

    def body(*refs):
        gather_kernel(row_count, col_count, *refs)

    return pl.pallas_call(
        body,
        out_shape=(
            pltpu.VMEM((height, width), jnp.float32),
            pltpu.VMEM((2, row_count, depth, width), jnp.float32),
            pltpu.VMEM((row_count, depth, width), jnp.float32),
        ),
        in_specs=[vmem, smem, smem, smem, vmem, vmem],
        out_specs=(vmem, vmem, vmem),
        scratch_shapes=[
            pltpu.VMEM((rows, order_full), jnp.float32),
            pltpu.VMEM((3 * depth, width), jnp.bfloat16),
            dma((col_count,)),
            dma((col_count,)),
            dma((row_count,)),
            dma((row_count,)),
            dma((row_count, col_count)),
            dma((row_count,)),
            dma((row_count,)),
            dma((row_count, col_count)),
            dma((row_count,)),
            dma((row_count,)),
        ],
        compiler_params=pltpu.CompilerParams(
            collective_id=0, has_side_effects=True, vmem_limit_bytes=VMEM_GRANT
        ),
    )(green, noise, data_set, set_scale, stiff, cell)


def finish_kernel(row_count, slots, acc, rowp, col, out, stage, right, sems):
    row = lax.axis_index("row")
    plane = plane_at(row, row_count - 1, row_count)
    height, width = acc.shape
    strip = stage.shape[1]
    load_right(col, plane, right)

    def copy(index, slot):
        start = pl.multiple_of(index * strip, LANES)
        return pltpu.make_async_copy(stage.at[slot], out.at[pl.ds(start, strip), :], sems.at[slot])

    count = height // strip

    @pl.loop(0, count)
    def _(index):
        slot = lax.rem(index, slots)

        @pl.when(index >= slots)
        def _():
            copy(index - slots, slot).wait()

        start = pl.multiple_of(index * strip, LANES)
        left = strip_left(rowp, plane, start, strip)

        stage[slot] = acc[pl.ds(start, strip), :] + contract_rows(left, right[...])
        copy(index, slot).start()

    for back in range(slots):
        index = count - slots + back
        copy(index, index % slots).wait()


def finish(row_count, acc, rowp, col):
    height, width = acc.shape
    depth = col.shape[1]
    vmem = pl.BlockSpec(memory_space=pltpu.VMEM)
    strip = min(height, 256)
    slots = 4

    def body(*refs):
        finish_kernel(row_count, slots, *refs)

    return pl.pallas_call(
        body,
        out_shape=jax.ShapeDtypeStruct((height, width), jnp.float32),
        in_specs=[vmem, vmem, vmem],
        out_specs=pl.BlockSpec(memory_space=pl.ANY),
        scratch_shapes=[
            pltpu.VMEM((slots, strip, width), jnp.float32),
            pltpu.VMEM((3 * depth, width), jnp.bfloat16),
            pltpu.SemaphoreType.DMA((slots,)),
        ],
        compiler_params=pltpu.CompilerParams(vmem_limit_bytes=VMEM_GRANT),
    )(*(pltpu.with_memory_space_constraint(array, pltpu.VMEM) for array in (acc, rowp, col)))


def per_device(green, noise_precision, data_set, set_scale, stiffness, patch_cell):
    row_count = lax.axis_size("row")
    col_count = lax.axis_size("col")
    lines = stiffness.shape[0] // LANES
    acc, rowp, col = gather_and_sum(
        row_count,
        col_count,
        green,
        noise_precision,
        data_set,
        set_scale,
        stiffness.reshape(lines, LANES),
        patch_cell.reshape(lines, LANES),
    )
    return finish(row_count, acc, rowp, col)


def solution(mesh):
    placed = (P(("row", "col"), None), P(("row", "col")), P(("row", "col")), P(), P(), P())
    return jax.shard_map(
        per_device, mesh=mesh, in_specs=placed, out_specs=P("row", "col"), check_vma=False
    )
```

```python
import jax
import jax.numpy as jnp
from jax import lax
from jax.experimental import pallas as pl
from jax.experimental.pallas import tpu as pltpu
from jax.sharding import PartitionSpec as P

NSTRIKE = 128
NDIP = 64
LANES = 128
VMEM_GRANT = 19 * 2**20
MESH = pl.DeviceIdType.MESH


def xor(value, other, count):
    total = 0
    bit = 1
    while bit < count:
        total = total + ((value // bit) % 2 + (other // bit) % 2) % 2 * bit
        bit *= 2
    return total


def ring_chip(place, chips):
    return jnp.where(place < chips // 2, place, chips + chips // 2 - 1 - place)


def plane_at(row, order, row_count):
    low = jnp.where(order % 2 == 1, row - (order + 1) // 2, row + order // 2)
    near = jnp.minimum(row, row_count - 1 - row)
    far = jnp.where(row < row_count - 1 - row, order, row_count - 1 - order)
    return jnp.where(order <= 2 * near, low, far)


def split_two(values):
    high = values.astype(jnp.bfloat16)
    low = (values - high.astype(jnp.float32)).astype(jnp.bfloat16)
    return high, low


def split_three(values):
    high = values.astype(jnp.bfloat16)
    rest = values - high.astype(jnp.float32)
    middle = rest.astype(jnp.bfloat16)
    low = (rest - middle.astype(jnp.float32)).astype(jnp.bfloat16)
    return high, middle, low


def contract_rows(left, right):
    return lax.dot_general(left, right, (((0,), (0,)), ((), ())), preferred_element_type=jnp.float32)


def load_right(col, planes, right):
    depth = col.shape[1]
    for index, plane in enumerate(planes):
        high, low = split_two(col[plane])
        for part, values in enumerate((high, high, low)):
            right[pl.ds((3 * index + part) * depth, depth), :] = values


def strip_left(rowp, planes, start, height):
    width = rowp.shape[3]
    half = start // width
    first = pl.multiple_of(start % width, LANES)
    parts = []
    for plane in planes:
        high, low = split_two(rowp[half, plane, :, pl.ds(first, height)])
        parts += [high, low, high]
    return jnp.concatenate(parts, axis=0)


def code_of(cells):
    return ((cells // NDIP) * (2 * NDIP) + cells % NDIP).astype(jnp.float32)


def hot_strike(cells):
    ids = lax.broadcasted_iota(jnp.int32, (NSTRIKE, LANES), 0)
    return jnp.where(ids == cells // NDIP, 1.0, 0.0)


def hot_dip(cells):
    ids = lax.broadcasted_iota(jnp.int32, (LANES, LANES), 0)
    return ids == cells % NDIP


def degree_grid(stiff, cell):
    group = 8

    def add(step, total):
        strikes = []
        parts = ([], [], [])
        for inner in range(group):
            cells = cell[pl.ds(step * group + inner, 1), :]
            strikes.append(hot_strike(cells).astype(jnp.bfloat16))
            chosen = jnp.where(hot_dip(cells), stiff[pl.ds(step * group + inner, 1), :], 0.0)
            for part, values in zip(parts, split_three(chosen)):
                part.append(values)
        tables = jnp.concatenate([jnp.concatenate(part, axis=1) for part in parts], axis=0)
        return total + lax.dot_general(
            jnp.concatenate(strikes, axis=1),
            tables,
            (((1,), (1,)), ((), ())),
            preferred_element_type=jnp.float32,
        )

    sums = lax.fori_loop(0, cell.shape[0] // group, add, jnp.zeros((NSTRIKE, 3 * LANES), jnp.float32))
    grid = sums[:, :LANES] + sums[:, LANES : 2 * LANES] + sums[:, 2 * LANES :]
    strike_ids = lax.broadcasted_iota(jnp.int32, (NSTRIKE, LANES), 0)
    dip_ids = lax.broadcasted_iota(jnp.int32, (NSTRIKE, LANES), 1)
    degree = jnp.where(strike_ids < NSTRIKE - 1, 0.5 * (grid + pltpu.roll(grid, NSTRIKE - 1, 0)), 0.0)
    degree = degree + jnp.where(strike_ids > 0, 0.5 * (grid + pltpu.roll(grid, 1, 0)), 0.0)
    degree = degree + jnp.where(dip_ids < NDIP - 1, 0.5 * (grid + pltpu.roll(grid, LANES - 1, 1)), 0.0)
    degree = degree + jnp.where(dip_ids > 0, 0.5 * (grid + pltpu.roll(grid, 1, 1)), 0.0)
    return degree


def degree_line(parts, cells):
    strike = hot_strike(cells).astype(jnp.bfloat16)
    table = contract_rows(parts[0], strike) + contract_rows(parts[1], strike) + contract_rows(parts[2], strike)
    return jnp.sum(jnp.where(hot_dip(cells), table, 0.0), axis=0, keepdims=True)


def prior_strip(stiff, cell, acc, row_line, col_line, start, height, same):
    width = acc.shape[1]

    @pl.when(same)
    def _():
        @pl.loop(0, height // LANES)
        def _(block):
            first = pl.multiple_of(start + block * LANES, LANES)
            line = row_line + first // LANES
            full = (LANES, LANES)
            row_code = jnp.broadcast_to(code_of(cell[pl.ds(line, 1), :]), full).T
            row_half = jnp.broadcast_to(-0.5 * stiff[pl.ds(line, 1), :], full).T
            for place in range(width // LANES):
                other = col_line + place
                apart = jnp.abs(row_code - code_of(cell[pl.ds(other, 1), :]))
                edge = row_half - 0.5 * stiff[pl.ds(other, 1), :]
                near = (apart == 1.0) | (apart == 2.0 * NDIP)
                acc[pl.ds(first, LANES), pl.ds(place * LANES, LANES)] = jnp.where(near, edge, 0.0)

    @pl.when(jnp.logical_not(same))
    def _():
        acc[pl.ds(start, height), :] = jnp.zeros((height, width), jnp.float32)


def gather_kernel(
    row_count,
    col_count,
    green,
    noise,
    data_set,
    set_scale,
    stiff,
    cell,
    acc,
    rowp,
    col,
    scaled,
    right,
    send_plane,
    recv_plane,
    send_up,
    send_down,
    recv_z,
    send_cw,
    send_ccw,
    recv_ring,
    send_core,
    recv_core,
):
    row = lax.axis_index("row")
    me = lax.axis_index("col")
    core = me % 2
    chip = me // 2
    chips = col_count // 2
    rows, order_full = green.shape
    height, width = acc.shape
    patches = stiff.shape[0] * LANES
    owner = chip == row
    home = 2 * row + core
    partner = 2 * chip + 1 - core
    place = ring_chip(chip, chips)
    hop_cw = lax.rem(place - ring_chip(row, chips) + chips, chips)
    hop_ccw = lax.rem(chips - hop_cw, chips)
    next_cw = 2 * ring_chip(lax.rem(place + 1, chips), chips) + core
    next_ccw = 2 * ring_chip(lax.rem(place + chips - 1, chips), chips) + core
    has_up = row + 1 < row_count
    has_down = row > 0
    above = jnp.minimum(row + 1, row_count - 1)
    below = jnp.maximum(row - 1, 0)

    barrier = pltpu.get_barrier_semaphore()
    for step in range(1, col_count):
        pl.semaphore_signal(barrier, inc=1, device_id=(row, xor(me, step, col_count)), device_id_type=MESH)

    @pl.when(has_up)
    def _():
        pl.semaphore_signal(barrier, inc=1, device_id=(above, me), device_id_type=MESH)

    @pl.when(has_down)
    def _():
        pl.semaphore_signal(barrier, inc=1, device_id=(below, me), device_id_type=MESH)

    row_ids = lax.broadcasted_iota(jnp.int32, (rows, LANES), 0)
    weight = jnp.zeros((rows, LANES), jnp.float32)
    for entry in range(rows):
        weight = jnp.where(row_ids == entry, noise[entry] * set_scale[data_set[entry]], weight)
    factor = jnp.sqrt(weight)

    @pl.loop(0, order_full // LANES)
    def _(step):
        lanes = pl.ds(pl.multiple_of(step * LANES, LANES), LANES)
        scaled[:, lanes] = green[:, lanes] * factor

    def slab(index):
        return pl.ds(pl.multiple_of(index * rows, rows), rows)

    own = pl.ds(pl.multiple_of(me * width, LANES), width)
    col[row, slab(me), :] = scaled[:, own]
    pl.semaphore_wait(barrier, col_count - 1 + has_up.astype(jnp.int32) + has_down.astype(jnp.int32))

    def plane_copy(step):
        target = xor(me, step, col_count)
        return pltpu.make_async_remote_copy(
            src_ref=scaled.at[:, pl.ds(pl.multiple_of(target * width, LANES), width)],
            dst_ref=col.at[row, slab(me), :],
            send_sem=send_plane.at[step],
            recv_sem=recv_plane.at[step],
            device_id=(row, target),
            device_id_type=MESH,
        )

    for step in range(1, col_count):
        plane_copy(step).start()

    def z_copy(plane, step, up):
        where = slab(xor(me, step, col_count))
        return pltpu.make_async_remote_copy(
            src_ref=col.at[plane, where, :],
            dst_ref=col.at[plane, where, :],
            send_sem=send_up.at[plane] if up else send_down.at[plane],
            recv_sem=recv_z.at[plane, step],
            device_id=(above if up else below, me),
            device_id_type=MESH,
        )

    def ring_copy(plane, step, clockwise, source):
        where = slab(xor(home, step, col_count))
        return pltpu.make_async_remote_copy(
            src_ref=source.at[plane, where, :],
            dst_ref=rowp.at[core, plane, where, :],
            send_sem=send_cw.at[plane] if clockwise else send_ccw.at[plane],
            recv_sem=recv_ring.at[plane, step],
            device_id=(row, next_cw if clockwise else next_ccw),
            device_id_type=MESH,
        )

    def core_copy(plane, step, source):
        where = slab(xor(home, step, col_count))
        return pltpu.make_async_remote_copy(
            src_ref=source.at[plane, where, :],
            dst_ref=rowp.at[core, plane, where, :],
            send_sem=send_core.at[plane],
            recv_sem=recv_core.at[plane],
            device_id=(row, partner),
            device_id_type=MESH,
        )

    def reach(distance, step):
        around = jnp.where(distance == row_count - 1, chips // 2, chips - 1)
        beside = jnp.where(distance == row_count - 1, chips // 2 - 1, 0)
        return jnp.where(step % 2 == 0, around, beside)

    def arrived(plane, step, distance):
        @pl.when(has_up & (plane <= row))
        def _():
            z_copy(plane, step, True).start()

        @pl.when(has_down & (plane >= row))
        def _():
            z_copy(plane, step, False).start()

        @pl.when(owner)
        def _():
            clockwise = reach(distance, step)

            @pl.when(clockwise > 0)
            def _():
                ring_copy(plane, step, True, col).start()

            @pl.when(clockwise < chips - 1)
            def _():
                ring_copy(plane, step, False, col).start()

            core_copy(plane, step, col).start()
            where = slab(xor(home, step, col_count))
            rowp[core, plane, where, :] = col[plane, where, :]

    held = rowp.at[core]

    def ring_step(plane, step, clockwise, onward):
        ring_copy(plane, step, clockwise, held).wait_recv()

        @pl.when(onward)
        def _():
            ring_copy(plane, step, clockwise, held).start()

        core_copy(plane, step, held).start()

    def both_sides(distance, act):
        @pl.when(row - distance >= 0)
        def _():
            act(row - distance)

        @pl.when((distance > 0) & (row + distance < row_count))
        def _():
            act(row + distance)

    def wait_core(plane):
        whole = rowp.at[1 - core, plane]
        pltpu.make_async_remote_copy(
            src_ref=whole,
            dst_ref=whole,
            send_sem=send_core.at[plane],
            recv_sem=recv_core.at[plane],
            device_id=(row, partner),
            device_id_type=MESH,
        ).wait_recv()

    lag = 2 * (chips - 1)
    steps = row_count * col_count
    strip = height // col_count
    inner = has_up & has_down
    behind = jnp.where(inner, 0, 0)
    same = (row * height) // patches == (me * width) // patches
    row_line = lax.rem(row * height, patches) // LANES
    col_line = lax.rem(me * width, patches) // LANES

    @pl.loop(0, steps + lag + 2)
    def _(now):
        distance = now // col_count
        step = lax.rem(now, col_count)

        @pl.when((now > 0) & (now < col_count))
        def _():
            pltpu.make_async_remote_copy(
                src_ref=col.at[row, slab(xor(me, step, col_count)), :],
                dst_ref=col.at[row, slab(xor(me, step, col_count)), :],
                send_sem=send_plane.at[step],
                recv_sem=recv_plane.at[step],
                device_id=(row, partner),
                device_id_type=MESH,
            ).wait_recv()

        @pl.when(now < steps)
        def _():
            def receive(plane):
                @pl.when(now >= col_count)
                def _():
                    z_copy(plane, step, True).wait_recv()

                arrived(plane, step, distance)

            both_sides(distance, receive)

        def ring_turn(hop, clockwise, behind, first, last):
            late = now - 2 * hop - behind
            far = late // col_count
            turn = lax.rem(late, col_count)
            limit = reach(far, turn)
            limit = limit if clockwise else chips - 1 - limit

            @pl.when((hop > 0) & (late >= first) & (late < last) & (hop <= limit))
            def _():
                both_sides(far, lambda plane: ring_step(plane, turn, clockwise, hop < limit))

        for hop, clockwise in ((hop_cw, True), (hop_ccw, False)):
            ring_turn(hop, clockwise, 0, 0, col_count)
            ring_turn(hop, clockwise, behind, col_count, steps)

        @pl.when((now >= col_count) & (now < 2 * col_count))
        def _():
            prior_strip(stiff, cell, acc, row_line, col_line, pl.multiple_of(step * strip, LANES), strip, same)

        @pl.when((now == 2 * col_count) & owner)
        def _():
            parts = split_three(degree_grid(stiff, cell))
            corner = lax.broadcasted_iota(jnp.int32, (LANES, LANES), 0) == lax.broadcasted_iota(
                jnp.int32, (LANES, LANES), 1
            )

            @pl.loop(0, width // LANES)
            def _(block):
                line = degree_line(parts, cell[pl.ds(col_line + block, 1), :])
                across = pl.ds(pl.multiple_of(block * LANES, LANES), LANES)
                down = pl.ds(pl.multiple_of(core * width + block * LANES, LANES), LANES)
                acc[down, across] = acc[down, across] + jnp.where(corner, line, 0.0)

        def add_planes(begin, orders, strip):
            part = now - begin

            @pl.when((part >= 0) & (part * strip < height))
            def _():
                planes = [plane_at(row, order, row_count) for order in orders]

                @pl.when(part == 0)
                def _():
                    for plane in planes:
                        wait_core(plane)
                    load_right(col, planes, right)

                piece = min(strip, 4 * LANES)
                used = right.at[pl.ds(0, 3 * len(planes) * col.shape[1]), :]

                @pl.loop(0, strip // piece)
                def _(block):
                    start = pl.multiple_of(part * strip + block * piece, LANES)
                    left = strip_left(rowp, planes, start, piece)
                    acc[pl.ds(start, piece), :] = acc[pl.ds(start, piece), :] + contract_rows(left, used[...])

        if row_count == 4:
            first = jnp.where(inner, 1, 0)
            add_planes(2 * col_count + lag + behind, (first, first + 1), strip)
            add_planes(jnp.where(inner, 2 * col_count, 3 * col_count + lag), (jnp.where(inner, 0, 2),), 2 * strip)
        else:
            order = jnp.clip((now - lag - 2) // col_count - 1, 0, row_count - 2)
            add_planes((order + 1) * col_count + lag + 2, (order,), strip)

    wait_core(plane_at(row, row_count - 1, row_count))

    for step in range(1, col_count):
        plane_copy(step).wait_send()

    @pl.loop(0, row_count)
    def _(plane):
        whole = col.at[plane]
        half = whole.at[pl.ds(0, whole.shape[0] // 2), :]

        def sent(ref, sem):
            pltpu.make_async_remote_copy(
                src_ref=ref,
                dst_ref=ref,
                send_sem=sem,
                recv_sem=recv_core.at[plane],
                device_id=(row, partner),
                device_id_type=MESH,
            ).wait_send()

        sent(whole, send_core.at[plane])

        @pl.when(has_up & (plane <= row))
        def _():
            sent(whole, send_up.at[plane])

        @pl.when(has_down & (plane >= row))
        def _():
            sent(whole, send_down.at[plane])

        for step in range(2):
            limit = reach(jnp.abs(plane - row), step)

            @pl.when(hop_cw < limit)
            def _():
                sent(half, send_cw.at[plane])

            @pl.when(hop_ccw < chips - 1 - limit)
            def _():
                sent(half, send_ccw.at[plane])


def gather_and_sum(row_count, col_count, green, noise, data_set, set_scale, stiff, cell):
    rows, order_full = green.shape
    height = order_full // row_count
    width = order_full // col_count
    depth = col_count * rows
    vmem = pl.BlockSpec(memory_space=pltpu.VMEM)
    smem = pl.BlockSpec(memory_space=pltpu.SMEM)
    dma = pltpu.SemaphoreType.DMA

    def body(*refs):
        gather_kernel(row_count, col_count, *refs)

    return pl.pallas_call(
        body,
        out_shape=(
            pltpu.VMEM((height, width), jnp.float32),
            pltpu.VMEM((2, row_count, depth, width), jnp.float32),
            pltpu.VMEM((row_count, depth, width), jnp.float32),
        ),
        in_specs=[vmem, smem, smem, smem, vmem, vmem],
        out_specs=(vmem, vmem, vmem),
        scratch_shapes=[
            pltpu.VMEM((rows, order_full), jnp.float32),
            pltpu.VMEM((6 * depth, width), jnp.bfloat16),
            dma((col_count,)),
            dma((col_count,)),
            dma((row_count,)),
            dma((row_count,)),
            dma((row_count, col_count)),
            dma((row_count,)),
            dma((row_count,)),
            dma((row_count, col_count)),
            dma((row_count,)),
            dma((row_count,)),
        ],
        compiler_params=pltpu.CompilerParams(
            collective_id=0, has_side_effects=True, vmem_limit_bytes=VMEM_GRANT
        ),
    )(green, noise, data_set, set_scale, stiff, cell)


def finish_kernel(row_count, slots, acc, rowp, col, out, stage, right, sems):
    row = lax.axis_index("row")
    plane = plane_at(row, row_count - 1, row_count)
    height, width = acc.shape
    strip = stage.shape[1]
    load_right(col, (plane,), right)

    def copy(index, slot):
        start = pl.multiple_of(index * strip, LANES)
        return pltpu.make_async_copy(stage.at[slot], out.at[pl.ds(start, strip), :], sems.at[slot])

    count = height // strip

    @pl.loop(0, count)
    def _(index):
        slot = lax.rem(index, slots)

        @pl.when(index >= slots)
        def _():
            copy(index - slots, slot).wait()

        start = pl.multiple_of(index * strip, LANES)
        left = strip_left(rowp, (plane,), start, strip)

        stage[slot] = acc[pl.ds(start, strip), :] + contract_rows(left, right[...])
        copy(index, slot).start()

    for back in range(slots):
        index = count - slots + back
        copy(index, index % slots).wait()


def finish(row_count, acc, rowp, col):
    height, width = acc.shape
    depth = col.shape[1]
    vmem = pl.BlockSpec(memory_space=pltpu.VMEM)
    strip = min(height, 512)
    slots = 3

    def body(*refs):
        finish_kernel(row_count, slots, *refs)

    return pl.pallas_call(
        body,
        out_shape=jax.ShapeDtypeStruct((height, width), jnp.float32),
        in_specs=[vmem, vmem, vmem],
        out_specs=pl.BlockSpec(memory_space=pl.ANY),
        scratch_shapes=[
            pltpu.VMEM((slots, strip, width), jnp.float32),
            pltpu.VMEM((3 * depth, width), jnp.bfloat16),
            pltpu.SemaphoreType.DMA((slots,)),
        ],
        compiler_params=pltpu.CompilerParams(vmem_limit_bytes=VMEM_GRANT),
    )(*(pltpu.with_memory_space_constraint(array, pltpu.VMEM) for array in (acc, rowp, col)))


def per_device(green, noise_precision, data_set, set_scale, stiffness, patch_cell):
    row_count = lax.axis_size("row")
    col_count = lax.axis_size("col")
    lines = stiffness.shape[0] // LANES
    acc, rowp, col = gather_and_sum(
        row_count,
        col_count,
        green,
        noise_precision,
        data_set,
        set_scale,
        stiffness.reshape(lines, LANES),
        patch_cell.reshape(lines, LANES),
    )
    return finish(row_count, acc, rowp, col)


def solution(mesh):
    placed = (P(("row", "col"), None), P(("row", "col")), P(("row", "col")), P(), P(), P())
    return jax.shard_map(
        per_device, mesh=mesh, in_specs=placed, out_specs=P("row", "col"), check_vma=False
    )
```

```python
import jax
import jax.numpy as jnp
from jax import lax
from jax.experimental import pallas as pl
from jax.experimental.pallas import tpu as pltpu
from jax.sharding import PartitionSpec as P

NSTRIKE = 128
NDIP = 64
LANES = 128
VMEM_GRANT = 19 * 2**20
MESH = pl.DeviceIdType.MESH


def xor(value, other, count):
    total = 0
    bit = 1
    while bit < count:
        total = total + ((value // bit) % 2 + (other // bit) % 2) % 2 * bit
        bit *= 2
    return total


def ring_chip(place, chips):
    return jnp.where(place < chips // 2, place, chips + chips // 2 - 1 - place)


def plane_at(row, order, row_count):
    low = jnp.where(order % 2 == 1, row - (order + 1) // 2, row + order // 2)
    near = jnp.minimum(row, row_count - 1 - row)
    far = jnp.where(row < row_count - 1 - row, order, row_count - 1 - order)
    return jnp.where(order <= 2 * near, low, far)


def split_two(values):
    high = values.astype(jnp.bfloat16)
    low = (values - high.astype(jnp.float32)).astype(jnp.bfloat16)
    return high, low


def split_three(values):
    high = values.astype(jnp.bfloat16)
    rest = values - high.astype(jnp.float32)
    middle = rest.astype(jnp.bfloat16)
    low = (rest - middle.astype(jnp.float32)).astype(jnp.bfloat16)
    return high, middle, low


def contract_rows(left, right):
    return lax.dot_general(left, right, (((0,), (0,)), ((), ())), preferred_element_type=jnp.float32)


def load_right(col, planes, right, terms=3):
    depth = col.shape[1]
    for index, plane in enumerate(planes):
        high, low = split_two(col[plane])
        for part, values in enumerate((high, high, low)[:terms]):
            right[pl.ds((terms * index + part) * depth, depth), :] = values


def strip_left(rowp, planes, start, height, terms=3):
    width = rowp.shape[3]
    half = start // width
    first = pl.multiple_of(start % width, LANES)
    parts = []
    for plane in planes:
        high, low = split_two(rowp[half, plane, :, pl.ds(first, height)])
        parts += [high, low, high][:terms]
    return jnp.concatenate(parts, axis=0)


def code_of(cells):
    return ((cells // NDIP) * (2 * NDIP) + cells % NDIP).astype(jnp.float32)


def hot_strike(cells):
    ids = lax.broadcasted_iota(jnp.int32, (NSTRIKE, LANES), 0)
    return jnp.where(ids == cells // NDIP, 1.0, 0.0)


def hot_dip(cells):
    ids = lax.broadcasted_iota(jnp.int32, (LANES, LANES), 0)
    return ids == cells % NDIP


def degree_grid(stiff, cell):
    group = 8

    def add(step, total):
        strikes = []
        parts = ([], [], [])
        for inner in range(group):
            cells = cell[pl.ds(step * group + inner, 1), :]
            strikes.append(hot_strike(cells).astype(jnp.bfloat16))
            chosen = jnp.where(hot_dip(cells), stiff[pl.ds(step * group + inner, 1), :], 0.0)
            for part, values in zip(parts, split_three(chosen)):
                part.append(values)
        tables = jnp.concatenate([jnp.concatenate(part, axis=1) for part in parts], axis=0)
        return total + lax.dot_general(
            jnp.concatenate(strikes, axis=1),
            tables,
            (((1,), (1,)), ((), ())),
            preferred_element_type=jnp.float32,
        )

    sums = lax.fori_loop(0, cell.shape[0] // group, add, jnp.zeros((NSTRIKE, 3 * LANES), jnp.float32))
    grid = sums[:, :LANES] + sums[:, LANES : 2 * LANES] + sums[:, 2 * LANES :]
    strike_ids = lax.broadcasted_iota(jnp.int32, (NSTRIKE, LANES), 0)
    dip_ids = lax.broadcasted_iota(jnp.int32, (NSTRIKE, LANES), 1)
    degree = jnp.where(strike_ids < NSTRIKE - 1, 0.5 * (grid + pltpu.roll(grid, NSTRIKE - 1, 0)), 0.0)
    degree = degree + jnp.where(strike_ids > 0, 0.5 * (grid + pltpu.roll(grid, 1, 0)), 0.0)
    degree = degree + jnp.where(dip_ids < NDIP - 1, 0.5 * (grid + pltpu.roll(grid, LANES - 1, 1)), 0.0)
    degree = degree + jnp.where(dip_ids > 0, 0.5 * (grid + pltpu.roll(grid, 1, 1)), 0.0)
    return degree


def degree_line(parts, cells):
    strike = hot_strike(cells).astype(jnp.bfloat16)
    table = contract_rows(parts[0], strike) + contract_rows(parts[1], strike) + contract_rows(parts[2], strike)
    return jnp.sum(jnp.where(hot_dip(cells), table, 0.0), axis=0, keepdims=True)


def prior_strip(stiff, cell, acc, row_line, col_line, start, height, same):
    width = acc.shape[1]

    @pl.when(same)
    def _():
        @pl.loop(0, height // LANES)
        def _(block):
            first = pl.multiple_of(start + block * LANES, LANES)
            line = row_line + first // LANES
            full = (LANES, LANES)
            row_code = jnp.broadcast_to(code_of(cell[pl.ds(line, 1), :]), full).T
            row_half = jnp.broadcast_to(-0.5 * stiff[pl.ds(line, 1), :], full).T
            for place in range(width // LANES):
                other = col_line + place
                apart = jnp.abs(row_code - code_of(cell[pl.ds(other, 1), :]))
                edge = row_half - 0.5 * stiff[pl.ds(other, 1), :]
                near = (apart == 1.0) | (apart == 2.0 * NDIP)
                acc[pl.ds(first, LANES), pl.ds(place * LANES, LANES)] = jnp.where(near, edge, 0.0)

    @pl.when(jnp.logical_not(same))
    def _():
        acc[pl.ds(start, height), :] = jnp.zeros((height, width), jnp.float32)


def lone_order(row, row_count):
    return jnp.where((row > 0) & (row < row_count - 1), 0, 2)


def gather_kernel(
    row_count,
    col_count,
    green,
    noise,
    data_set,
    set_scale,
    stiff,
    cell,
    acc,
    rowp,
    col,
    scaled,
    right,
    send_plane,
    recv_plane,
    send_up,
    send_down,
    recv_z,
    send_cw,
    send_ccw,
    recv_ring,
    send_core,
    recv_core,
):
    row = lax.axis_index("row")
    me = lax.axis_index("col")
    core = me % 2
    chip = me // 2
    chips = col_count // 2
    rows, order_full = green.shape
    height, width = acc.shape
    patches = stiff.shape[0] * LANES
    owner = chip == row
    home = 2 * row + core
    partner = 2 * chip + 1 - core
    place = ring_chip(chip, chips)
    hop_cw = lax.rem(place - ring_chip(row, chips) + chips, chips)
    hop_ccw = lax.rem(chips - hop_cw, chips)
    next_cw = 2 * ring_chip(lax.rem(place + 1, chips), chips) + core
    next_ccw = 2 * ring_chip(lax.rem(place + chips - 1, chips), chips) + core
    has_up = row + 1 < row_count
    has_down = row > 0
    above = jnp.minimum(row + 1, row_count - 1)
    below = jnp.maximum(row - 1, 0)

    barrier = pltpu.get_barrier_semaphore()
    for step in range(1, col_count):
        pl.semaphore_signal(barrier, inc=1, device_id=(row, xor(me, step, col_count)), device_id_type=MESH)

    @pl.when(has_up)
    def _():
        pl.semaphore_signal(barrier, inc=1, device_id=(above, me), device_id_type=MESH)

    @pl.when(has_down)
    def _():
        pl.semaphore_signal(barrier, inc=1, device_id=(below, me), device_id_type=MESH)

    row_ids = lax.broadcasted_iota(jnp.int32, (rows, LANES), 0)
    weight = jnp.zeros((rows, LANES), jnp.float32)
    for entry in range(rows):
        weight = jnp.where(row_ids == entry, noise[entry] * set_scale[data_set[entry]], weight)
    factor = jnp.sqrt(weight)

    @pl.loop(0, order_full // LANES)
    def _(step):
        lanes = pl.ds(pl.multiple_of(step * LANES, LANES), LANES)
        scaled[:, lanes] = green[:, lanes] * factor

    def slab(index):
        return pl.ds(pl.multiple_of(index * rows, rows), rows)

    own = pl.ds(pl.multiple_of(me * width, LANES), width)
    col[row, slab(me), :] = scaled[:, own]
    pl.semaphore_wait(barrier, col_count - 1 + has_up.astype(jnp.int32) + has_down.astype(jnp.int32))

    def plane_copy(step):
        target = xor(me, step, col_count)
        return pltpu.make_async_remote_copy(
            src_ref=scaled.at[:, pl.ds(pl.multiple_of(target * width, LANES), width)],
            dst_ref=col.at[row, slab(me), :],
            send_sem=send_plane.at[step],
            recv_sem=recv_plane.at[step],
            device_id=(row, target),
            device_id_type=MESH,
        )

    for step in range(1, col_count):
        plane_copy(step).start()

    def z_copy(plane, step, up):
        where = slab(xor(me, step, col_count))
        return pltpu.make_async_remote_copy(
            src_ref=col.at[plane, where, :],
            dst_ref=col.at[plane, where, :],
            send_sem=send_up.at[plane] if up else send_down.at[plane],
            recv_sem=recv_z.at[plane, step],
            device_id=(above if up else below, me),
            device_id_type=MESH,
        )

    def ring_copy(plane, step, clockwise, source):
        where = slab(xor(home, step, col_count))
        return pltpu.make_async_remote_copy(
            src_ref=source.at[plane, where, :],
            dst_ref=rowp.at[core, plane, where, :],
            send_sem=send_cw.at[plane] if clockwise else send_ccw.at[plane],
            recv_sem=recv_ring.at[plane, step],
            device_id=(row, next_cw if clockwise else next_ccw),
            device_id_type=MESH,
        )

    def core_copy(plane, step, source):
        where = slab(xor(home, step, col_count))
        return pltpu.make_async_remote_copy(
            src_ref=source.at[plane, where, :],
            dst_ref=rowp.at[core, plane, where, :],
            send_sem=send_core.at[plane],
            recv_sem=recv_core.at[plane],
            device_id=(row, partner),
            device_id_type=MESH,
        )

    def reach(distance, step):
        around = jnp.where(distance == row_count - 1, chips // 2, chips - 1)
        beside = jnp.where(distance == row_count - 1, chips // 2 - 1, 0)
        return jnp.where(step % 2 == 0, around, beside)

    def arrived(plane, step, distance):
        @pl.when(has_up & (plane <= row))
        def _():
            z_copy(plane, step, True).start()

        @pl.when(has_down & (plane >= row))
        def _():
            z_copy(plane, step, False).start()

        @pl.when(owner)
        def _():
            clockwise = reach(distance, step)

            @pl.when(clockwise > 0)
            def _():
                ring_copy(plane, step, True, col).start()

            @pl.when(clockwise < chips - 1)
            def _():
                ring_copy(plane, step, False, col).start()

            core_copy(plane, step, col).start()
            where = slab(xor(home, step, col_count))
            rowp[core, plane, where, :] = col[plane, where, :]

    held = rowp.at[core]

    def ring_step(plane, step, clockwise, onward):
        ring_copy(plane, step, clockwise, held).wait_recv()

        @pl.when(onward)
        def _():
            ring_copy(plane, step, clockwise, held).start()

        core_copy(plane, step, held).start()

    def both_sides(distance, act):
        @pl.when(row - distance >= 0)
        def _():
            act(row - distance)

        @pl.when((distance > 0) & (row + distance < row_count))
        def _():
            act(row + distance)

    def wait_core(plane):
        whole = rowp.at[1 - core, plane]
        pltpu.make_async_remote_copy(
            src_ref=whole,
            dst_ref=whole,
            send_sem=send_core.at[plane],
            recv_sem=recv_core.at[plane],
            device_id=(row, partner),
            device_id_type=MESH,
        ).wait_recv()

    lag = 2 * (chips - 1)
    steps = row_count * col_count
    strip = height // col_count
    inner = has_up & has_down
    behind = 0
    same = (row * height) // patches == (me * width) // patches
    row_line = lax.rem(row * height, patches) // LANES
    col_line = lax.rem(me * width, patches) // LANES

    @pl.loop(0, steps + lag + 2)
    def _(now):
        distance = now // col_count
        step = lax.rem(now, col_count)

        @pl.when((now > 0) & (now < col_count))
        def _():
            pltpu.make_async_remote_copy(
                src_ref=col.at[row, slab(xor(me, step, col_count)), :],
                dst_ref=col.at[row, slab(xor(me, step, col_count)), :],
                send_sem=send_plane.at[step],
                recv_sem=recv_plane.at[step],
                device_id=(row, partner),
                device_id_type=MESH,
            ).wait_recv()

        @pl.when(now < steps)
        def _():
            def receive(plane):
                @pl.when(now >= col_count)
                def _():
                    z_copy(plane, step, True).wait_recv()

                arrived(plane, step, distance)

            both_sides(distance, receive)

        def ring_turn(hop, clockwise, behind, first, last):
            late = now - 2 * hop - behind
            far = late // col_count
            turn = lax.rem(late, col_count)
            limit = reach(far, turn)
            limit = limit if clockwise else chips - 1 - limit

            @pl.when((hop > 0) & (late >= first) & (late < last) & (hop <= limit))
            def _():
                both_sides(far, lambda plane: ring_step(plane, turn, clockwise, hop < limit))

        for hop, clockwise in ((hop_cw, True), (hop_ccw, False)):
            ring_turn(hop, clockwise, 2, 0, col_count)
            ring_turn(hop, clockwise, behind, col_count, steps)

        @pl.when((now >= col_count) & (now < 2 * col_count))
        def _():
            prior_strip(stiff, cell, acc, row_line, col_line, pl.multiple_of(step * strip, LANES), strip, same)

        @pl.when((now == 2 * col_count) & owner)
        def _():
            parts = split_three(degree_grid(stiff, cell))
            corner = lax.broadcasted_iota(jnp.int32, (LANES, LANES), 0) == lax.broadcasted_iota(
                jnp.int32, (LANES, LANES), 1
            )

            @pl.loop(0, width // LANES)
            def _(block):
                line = degree_line(parts, cell[pl.ds(col_line + block, 1), :])
                across = pl.ds(pl.multiple_of(block * LANES, LANES), LANES)
                down = pl.ds(pl.multiple_of(core * width + block * LANES, LANES), LANES)
                acc[down, across] = acc[down, across] + jnp.where(corner, line, 0.0)

        def add_planes(begin, orders, strip, terms=3):
            part = now - begin

            @pl.when((part >= 0) & (part * strip < height))
            def _():
                planes = [plane_at(row, order, row_count) for order in orders]

                @pl.when(part == 0)
                def _():
                    for plane in planes:
                        wait_core(plane)
                    load_right(col, planes, right, terms)

                piece = min(strip, 4 * LANES)
                used = right.at[pl.ds(0, terms * len(planes) * col.shape[1]), :]

                @pl.loop(0, strip // piece)
                def _(block):
                    start = pl.multiple_of(part * strip + block * piece, LANES)
                    left = strip_left(rowp, planes, start, piece, terms)
                    acc[pl.ds(start, piece), :] = acc[pl.ds(start, piece), :] + contract_rows(left, used[...])

        if row_count == 4:
            first = jnp.where(inner, 1, 0)
            begin = jnp.where(inner, 2 * col_count + 0, 3 * col_count + lag)
            add_planes(2 * col_count + lag, (first, first + 1), strip)
            add_planes(begin, (lone_order(row, row_count),), 2 * strip, 2)
        else:
            order = jnp.clip((now - lag - 2) // col_count - 1, 0, row_count - 2)
            add_planes((order + 1) * col_count + lag + 2, (order,), strip)

    wait_core(plane_at(row, row_count - 1, row_count))

    for step in range(1, col_count):
        plane_copy(step).wait_send()

    @pl.loop(0, row_count)
    def _(plane):
        whole = col.at[plane]
        half = whole.at[pl.ds(0, whole.shape[0] // 2), :]

        def sent(ref, sem):
            pltpu.make_async_remote_copy(
                src_ref=ref,
                dst_ref=ref,
                send_sem=sem,
                recv_sem=recv_core.at[plane],
                device_id=(row, partner),
                device_id_type=MESH,
            ).wait_send()

        sent(whole, send_core.at[plane])

        @pl.when(has_up & (plane <= row))
        def _():
            sent(whole, send_up.at[plane])

        @pl.when(has_down & (plane >= row))
        def _():
            sent(whole, send_down.at[plane])

        for step in range(2):
            limit = reach(jnp.abs(plane - row), step)

            @pl.when(hop_cw < limit)
            def _():
                sent(half, send_cw.at[plane])

            @pl.when(hop_ccw < chips - 1 - limit)
            def _():
                sent(half, send_ccw.at[plane])


def gather_and_sum(row_count, col_count, green, noise, data_set, set_scale, stiff, cell):
    rows, order_full = green.shape
    height = order_full // row_count
    width = order_full // col_count
    depth = col_count * rows
    vmem = pl.BlockSpec(memory_space=pltpu.VMEM)
    smem = pl.BlockSpec(memory_space=pltpu.SMEM)
    dma = pltpu.SemaphoreType.DMA

    def body(*refs):
        gather_kernel(row_count, col_count, *refs)

    return pl.pallas_call(
        body,
        out_shape=(
            pltpu.VMEM((height, width), jnp.float32),
            pltpu.VMEM((2, row_count, depth, width), jnp.float32),
            pltpu.VMEM((row_count, depth, width), jnp.float32),
        ),
        in_specs=[vmem, smem, smem, smem, vmem, vmem],
        out_specs=(vmem, vmem, vmem),
        scratch_shapes=[
            pltpu.VMEM((rows, order_full), jnp.float32),
            pltpu.VMEM((6 * depth, width), jnp.bfloat16),
            dma((col_count,)),
            dma((col_count,)),
            dma((row_count,)),
            dma((row_count,)),
            dma((row_count, col_count)),
            dma((row_count,)),
            dma((row_count,)),
            dma((row_count, col_count)),
            dma((row_count,)),
            dma((row_count,)),
        ],
        compiler_params=pltpu.CompilerParams(
            collective_id=0, has_side_effects=True, vmem_limit_bytes=VMEM_GRANT
        ),
    )(green, noise, data_set, set_scale, stiff, cell)


def finish_kernel(row_count, slots, acc, rowp, col, out, stage, right, sems):
    row = lax.axis_index("row")
    plane = plane_at(row, row_count - 1, row_count)
    height, width = acc.shape
    strip = stage.shape[1]
    depth = col.shape[1]
    shared = row_count == 4
    load_right(col, (plane,), right)
    if shared:
        lone = plane_at(row, lone_order(row, row_count), row_count)
        right[pl.ds(3 * depth, depth), :] = split_two(col[lone])[1]

    def copy(index, slot):
        start = pl.multiple_of(index * strip, LANES)
        return pltpu.make_async_copy(stage.at[slot], out.at[pl.ds(start, strip), :], sems.at[slot])

    count = height // strip

    @pl.loop(0, count)
    def _(index):
        slot = lax.rem(index, slots)

        @pl.when(index >= slots)
        def _():
            copy(index - slots, slot).wait()

        start = pl.multiple_of(index * strip, LANES)
        left = strip_left(rowp, (plane,), start, strip)
        if shared:
            left = jnp.concatenate([left, strip_left(rowp, (lone,), start, strip, 1)], axis=0)

        stage[slot] = acc[pl.ds(start, strip), :] + contract_rows(left, right[...])
        copy(index, slot).start()

    for back in range(slots):
        index = count - slots + back
        copy(index, index % slots).wait()


def finish(row_count, acc, rowp, col):
    height, width = acc.shape
    depth = col.shape[1]
    vmem = pl.BlockSpec(memory_space=pltpu.VMEM)
    strip = min(height, 512)
    slots = 3

    def body(*refs):
        finish_kernel(row_count, slots, *refs)

    return pl.pallas_call(
        body,
        out_shape=jax.ShapeDtypeStruct((height, width), jnp.float32),
        in_specs=[vmem, vmem, vmem],
        out_specs=pl.BlockSpec(memory_space=pl.ANY),
        scratch_shapes=[
            pltpu.VMEM((slots, strip, width), jnp.float32),
            pltpu.VMEM(((4 if row_count == 4 else 3) * depth, width), jnp.bfloat16),
            pltpu.SemaphoreType.DMA((slots,)),
        ],
        compiler_params=pltpu.CompilerParams(vmem_limit_bytes=VMEM_GRANT),
    )(*(pltpu.with_memory_space_constraint(array, pltpu.VMEM) for array in (acc, rowp, col)))


def per_device(green, noise_precision, data_set, set_scale, stiffness, patch_cell):
    row_count = lax.axis_size("row")
    col_count = lax.axis_size("col")
    lines = stiffness.shape[0] // LANES
    acc, rowp, col = gather_and_sum(
        row_count,
        col_count,
        green,
        noise_precision,
        data_set,
        set_scale,
        stiffness.reshape(lines, LANES),
        patch_cell.reshape(lines, LANES),
    )
    return finish(row_count, acc, rowp, col)


def solution(mesh):
    placed = (P(("row", "col"), None), P(("row", "col")), P(("row", "col")), P(), P(), P())
    return jax.shard_map(
        per_device, mesh=mesh, in_specs=placed, out_specs=P("row", "col"), check_vma=False
    )
```
